16 devices in a mesh: cp: 2 (over z), fsdp: 8 (over y, x, core).
Axes of the slice: x: 2, y: 2, z: 2, core: 2. Of those that a mesh axis runs over, the one named last changes fastest.
Arguments:
- hidden_in: bfloat16 [256, 192, 1024], P('fsdp', 'cp')
- select_pos: int32 [256, 24], P('fsdp')
- w_router: bfloat16 [1024], P('fsdp')
- norm_attn: bfloat16 [2, 1024], P(None, 'fsdp')
- w_qkv: bfloat16 [2, 1024, 3, 16, 64], P(None, 'fsdp')
- w_out: bfloat16 [2, 1024, 1024], P(None, 'fsdp')
- norm_mlp: bfloat16 [2, 1024], P(None, 'fsdp')
- w_gate: bfloat16 [2, 1024, 4096], P(None, 'fsdp')
- w_up: bfloat16 [2, 1024, 4096], P(None, 'fsdp')
- w_down: bfloat16 [2, 4096, 1024], P(None, 'fsdp')
- d_out: bfloat16 [256, 192, 1024], P('fsdp', 'cp')
Outputs:
- output 1: bfloat16 [256, 192, 1024], P('fsdp', 'cp')
- output 2: bfloat16 [256, 192, 1024], P('fsdp', 'cp')
- output 3: bfloat16 [1024], P('fsdp')
- output 4: bfloat16 [2, 1024], P(None, 'fsdp')
- output 5: bfloat16 [2, 1024, 3, 16, 64], P(None, 'fsdp')
- output 6: bfloat16 [2, 1024, 1024], P(None, 'fsdp')
- output 7: bfloat16 [2, 1024], P(None, 'fsdp')
- output 8: bfloat16 [2, 1024, 4096], P(None, 'fsdp')
- output 9: bfloat16 [2, 1024, 4096], P(None, 'fsdp')
- output 10: bfloat16 [2, 4096, 1024], P(None, 'fsdp')
All inputs are finite; a program needn't handle non-finite values.
Results may differ from the reference program's by a relative error of at most 0.02.
Values are sent between devices in bfloat16 or wider.
A program may use at most 1 GiB of HBM per device.

```python
import jax
import jax.numpy as jnp
from jax import lax

D = 1024
HEADS = 16
FF = 4096
BATCH = 256
SEQ = 192

HEAD_DIM = D // HEADS
SELECT = SEQ // 8
EPS = 1e-5
ROPE_BASE = 10000.0


def draw_selection(key):
    key_noise, key_slope = jax.random.split(key)
    noise = jax.random.randint(key_noise, (BATCH, SEQ), 0, 4096)
    slope = jax.random.randint(key_slope, (BATCH, 1), -1024, 1025)
    position = jnp.arange(SEQ, dtype=jnp.int32)[None, :]
    score = noise + (slope * position) // SEQ + 1024
    distinct = score * SEQ + position
    top_vals, top_index = lax.top_k(distinct, SELECT)
    return jnp.sort(top_index, axis=1).astype(jnp.int32)


def normal_draw(key, shape, scale):
    return jax.random.normal(key, shape, jnp.float32) * scale


def setup_inputs(seed: int = 0) -> dict:
    keys = jax.random.split(jax.random.key(seed), 11)
    return {
        'hidden_in': normal_draw(keys[0], (BATCH, SEQ, D), 1.0).astype(jnp.bfloat16),
        'select_pos': draw_selection(keys[1]),
        'w_router': normal_draw(keys[2], (D,), D ** -0.5).astype(jnp.bfloat16),
        'norm_attn': (1.0 + normal_draw(keys[3], (2, D), 0.3)).astype(jnp.bfloat16),
        'w_qkv': normal_draw(keys[4], (2, D, 3, HEADS, HEAD_DIM), D ** -0.5).astype(jnp.bfloat16),
        'w_out': normal_draw(keys[5], (2, D, D), D ** -0.5).astype(jnp.bfloat16),
        'norm_mlp': (1.0 + normal_draw(keys[6], (2, D), 0.3)).astype(jnp.bfloat16),
        'w_gate': normal_draw(keys[7], (2, D, FF), D ** -0.5).astype(jnp.bfloat16),
        'w_up': normal_draw(keys[8], (2, D, FF), D ** -0.5).astype(jnp.bfloat16),
        'w_down': normal_draw(keys[9], (2, FF, D), FF ** -0.5).astype(jnp.bfloat16),
        'd_out': normal_draw(keys[10], (BATCH, SEQ, D), 1.0).astype(jnp.bfloat16),
    }


def rms_norm(values, gain):
    values_f = values.astype(jnp.float32)
    inv_rms = lax.rsqrt(jnp.mean(values_f * values_f, axis=-1, keepdims=True) + EPS)
    return (values_f * inv_rms * gain.astype(jnp.float32)).astype(jnp.bfloat16)


def rotate(values, positions):
    half = HEAD_DIM // 2
    inv_freq = ROPE_BASE ** (-jnp.arange(half, dtype=jnp.float32) / half)
    angles = positions.astype(jnp.float32)[:, None, None] * inv_freq
    cosine = jnp.cos(angles)
    sine = jnp.sin(angles)
    first = values[..., :half]
    second = values[..., half:]
    return jnp.concatenate([first * cosine - second * sine, second * cosine + first * sine], axis=-1)


def attend(q_rot, k_rot, v_rows, positions):
    scores = jnp.einsum('she,the->hst', q_rot.astype(jnp.float32), k_rot.astype(jnp.float32)) * HEAD_DIM ** -0.5
    allowed = positions[:, None] >= positions[None, :]
    scores = jnp.where(allowed[None], scores, -1e30)
    attn_probs = jax.nn.softmax(scores, axis=-1).astype(jnp.bfloat16)
    mixed = jnp.einsum('hst,the->she', attn_probs.astype(jnp.float32), v_rows.astype(jnp.float32))
    return mixed.astype(jnp.bfloat16)


def block(rows, positions, gain_attn, qkv_w, out_w, gain_mlp, gate_w, up_w, down_w):
    count = rows.shape[0]
    normed = rms_norm(rows, gain_attn)
    qkv_proj = jnp.dot(normed, qkv_w.reshape(D, 3 * D), preferred_element_type=jnp.float32).reshape(count, 3, HEADS, HEAD_DIM)
    q_rot = rotate(qkv_proj[:, 0], positions).astype(jnp.bfloat16)
    k_rot = rotate(qkv_proj[:, 1], positions).astype(jnp.bfloat16)
    v_rows = qkv_proj[:, 2].astype(jnp.bfloat16)
    attn_rows = attend(q_rot, k_rot, v_rows, positions).reshape(count, D)
    mixed = jnp.dot(attn_rows, out_w, preferred_element_type=jnp.float32)
    hidden = (rows.astype(jnp.float32) + mixed).astype(jnp.bfloat16)
    normed_mlp = rms_norm(hidden, gain_mlp)
    gate = jnp.dot(normed_mlp, gate_w, preferred_element_type=jnp.float32)
    upper = jnp.dot(normed_mlp, up_w, preferred_element_type=jnp.float32)
    activated = (jax.nn.silu(gate) * upper).astype(jnp.bfloat16)
    mlp_out = jnp.dot(activated, down_w, preferred_element_type=jnp.float32)
    return mixed, hidden, mlp_out


def sequence_forward(rows, picks, w_router, norm_attn, w_qkv, w_out, norm_mlp, w_gate, w_up, w_down):
    positions = jnp.arange(SEQ, dtype=jnp.int32)
    mixed, hidden, mlp_out = block(rows, positions, norm_attn[0], w_qkv[0], w_out[0], norm_mlp[0], w_gate[0], w_up[0], w_down[0])
    first_out = (hidden.astype(jnp.float32) + mlp_out).astype(jnp.bfloat16)
    chosen = first_out[picks]
    router = jnp.dot(chosen.astype(jnp.float32), w_router.astype(jnp.float32))
    mixed_two, unused_hidden, mlp_two = block(chosen, picks, norm_attn[1], w_qkv[1], w_out[1], norm_mlp[1], w_gate[1], w_up[1], w_down[1])
    delta = (mixed_two + mlp_two).astype(jnp.bfloat16)
    updated = (chosen.astype(jnp.float32) + router[:, None] * delta.astype(jnp.float32)).astype(jnp.bfloat16)
    return first_out.at[picks].set(updated)


sequence_saved = jax.checkpoint(sequence_forward)


def reference(hidden_in, select_pos, w_router, norm_attn, w_qkv, w_out, norm_mlp, w_gate, w_up, w_down, d_out):
    def run_layers(rows_all, router_w, gains_attn, qkv_w, out_w, gains_mlp, gate_w, up_w, down_w):
        def one_sequence(seq_pair):
            return sequence_saved(seq_pair[0], seq_pair[1], router_w.astype(jnp.bfloat16), gains_attn.astype(jnp.bfloat16), qkv_w.astype(jnp.bfloat16), out_w.astype(jnp.bfloat16), gains_mlp.astype(jnp.bfloat16), gate_w.astype(jnp.bfloat16), up_w.astype(jnp.bfloat16), down_w.astype(jnp.bfloat16))
        return lax.map(one_sequence, (rows_all, select_pos))
    result, pullback = jax.vjp(run_layers, hidden_in, w_router.astype(jnp.float32), norm_attn.astype(jnp.float32), w_qkv.astype(jnp.float32), w_out.astype(jnp.float32), norm_mlp.astype(jnp.float32), w_gate.astype(jnp.float32), w_up.astype(jnp.float32), w_down.astype(jnp.float32))
    cotangents = pullback(d_out)
    return (result, cotangents[0].astype(jnp.bfloat16), cotangents[1].astype(jnp.bfloat16), cotangents[2].astype(jnp.bfloat16), cotangents[3].astype(jnp.bfloat16), cotangents[4].astype(jnp.bfloat16), cotangents[5].astype(jnp.bfloat16), cotangents[6].astype(jnp.bfloat16), cotangents[7].astype(jnp.bfloat16), cotangents[8].astype(jnp.bfloat16))
```

```python
import jax
import jax.numpy as jnp
from jax import lax
from jax.experimental import pallas as pl
from jax.experimental.pallas import tpu as pltpu
from jax.sharding import PartitionSpec as P

EPS = 1e-5
ROPE_BASE = 10000.0
F32 = jnp.float32
BF16 = jnp.bfloat16

D = 1024
HEADS = 16
HEAD_DIM = 64
PAIR = 2 * HEAD_DIM
SLOTS = 2
ROWS = 96
SEQ = SLOTS * ROWS


def rms_norm(values, gain):
    values_f = values.astype(F32)
    inv_rms = lax.rsqrt(jnp.mean(values_f * values_f, axis=-1, keepdims=True) + EPS)
    return (values_f * inv_rms * gain).astype(BF16)


def gated(gate, upper):
    return (jax.nn.silu(gate) * upper).astype(BF16)


def swap_halves(part):
    lane = lax.broadcasted_iota(jnp.int32, part.shape, 1)
    return jnp.where(lane % HEAD_DIM < HEAD_DIM // 2, pltpu.roll(part, PAIR - HEAD_DIM // 2, 1), pltpu.roll(part, HEAD_DIM // 2, 1))


def qkv_kernel(x_ref, gain_ref, w_ref, cos_ref, sin_ref, n_ref, out_ref):
    x_f = x_ref[...].astype(F32)
    inv_rms = lax.rsqrt(jnp.mean(x_f * x_f, axis=-1, keepdims=True) + EPS)
    normed = (x_f * inv_rms * gain_ref[...]).astype(BF16)
    n_ref[...] = normed
    cosine = cos_ref[...]
    sine = sin_ref[...]
    width = 512
    for chunk in range(3 * D // width):
        acc = jnp.dot(normed, w_ref[:, chunk * width:(chunk + 1) * width], preferred_element_type=F32)
        if chunk * width < 2 * D:
            for j in range(width // PAIR):
                part = acc[:, j * PAIR:(j + 1) * PAIR]
                lo = chunk * width + j * PAIR
                out_ref[:, lo:lo + PAIR] = (part * cosine + swap_halves(part) * sine).astype(BF16)
        else:
            out_ref[:, chunk * width:(chunk + 1) * width] = acc.astype(BF16)


def qkv_project(x, gain, w, cosine, sine, block):
    rows = x.shape[0]
    return pl.pallas_call(
        qkv_kernel,
        grid=(rows // block,),
        in_specs=[
            pl.BlockSpec((block, D), lambda i: (i, 0)),
            pl.BlockSpec((1, D), lambda i: (0, 0)),
            pl.BlockSpec((D, 3 * D), lambda i: (0, 0)),
            pl.BlockSpec((block, PAIR), lambda i: (i, 0)),
            pl.BlockSpec((block, PAIR), lambda i: (i, 0)),
        ],
        out_specs=[pl.BlockSpec((block, D), lambda i: (i, 0)), pl.BlockSpec((block, 3 * D), lambda i: (i, 0))],
        out_shape=[jax.ShapeDtypeStruct((rows, D), BF16), jax.ShapeDtypeStruct((rows, 3 * D), BF16)],
        cost_estimate=pl.CostEstimate(flops=6 * rows * D * D, bytes_accessed=rows * D * 10 + 6 * D * D, transcendentals=rows),
        name='qkv_project',
    )(x, gain.reshape(1, D), w, cosine, sine)


def attention_bias(col_ref, row_ref):
    code_q = col_ref[0]
    code_k = row_ref[0]
    allowed = (code_k <= code_q) & ((code_k >> 8) == (code_q >> 8))
    return jnp.where(allowed, 0.0, -1e30).astype(F32)


def load_pair(ref, lo):
    return ref[:, 0, :, pl.ds(lo, PAIR)].reshape(SEQ, PAIR)


def side_mask(side):
    lane = lax.broadcasted_iota(jnp.int32, (1, PAIR), 1)
    return (lane // HEAD_DIM == side).astype(F32).astype(BF16)


def dot_nt(a, b):
    return lax.dot_general(a, b, (((1,), (1,)), ((), ())), preferred_element_type=F32)


def dot_tn(a, b):
    return lax.dot_general(a, b, (((0,), (0,)), ((), ())), preferred_element_type=F32)


def probabilities(query, keys, bias):
    scores = dot_nt(query, keys) * (HEAD_DIM ** -0.5) + bias
    top = jnp.max(scores, axis=-1, keepdims=True)
    expo = jnp.exp(scores - top)
    return expo / jnp.sum(expo, axis=-1, keepdims=True)


def attend_kernel(qkv_ref, col_ref, row_ref, o_ref):
    bias = attention_bias(col_ref, row_ref)

    def body(h, carry):
        lo = pl.multiple_of(h * PAIR, PAIR)
        query = load_pair(qkv_ref, lo)
        keys = load_pair(qkv_ref, pl.multiple_of(D + lo, PAIR))
        vals = load_pair(qkv_ref, pl.multiple_of(2 * D + lo, PAIR))
        out = jnp.zeros((SEQ, PAIR), F32)
        for side in range(2):
            mask = side_mask(side)
            probs = probabilities(query * mask, keys, bias).astype(BF16)
            out = out + jnp.dot(probs, vals * mask, preferred_element_type=F32)
        o_ref[:, 0, :, pl.ds(lo, PAIR)] = out.astype(BF16).reshape(SLOTS, ROWS, PAIR)
        return carry

    lax.fori_loop(0, HEADS // 2, body, 0)


def attend_back_kernel(qkv_ref, do_ref, col_ref, row_ref, cos_ref, sin_ref, out_ref):
    bias = attention_bias(col_ref, row_ref)
    cosine = cos_ref[:, 0].reshape(SEQ, PAIR)
    sine = sin_ref[:, 0].reshape(SEQ, PAIR)

    def unrotate(grad):
        part = grad.astype(BF16).astype(F32)
        return (part * cosine - swap_halves(part) * sine).astype(BF16).reshape(SLOTS, ROWS, PAIR)

    def body(h, carry):
        lo = pl.multiple_of(h * PAIR, PAIR)
        lo_k = pl.multiple_of(D + lo, PAIR)
        lo_v = pl.multiple_of(2 * D + lo, PAIR)
        query = load_pair(qkv_ref, lo)
        keys = load_pair(qkv_ref, lo_k)
        vals = load_pair(qkv_ref, lo_v)
        d_out = load_pair(do_ref, lo)
        d_query = jnp.zeros((SEQ, PAIR), F32)
        d_keys = jnp.zeros((SEQ, PAIR), F32)
        d_vals = jnp.zeros((SEQ, PAIR), F32)
        for side in range(2):
            mask = side_mask(side)
            query_s = query * mask
            d_out_s = d_out * mask
            probs = probabilities(query_s, keys, bias)
            d_probs = dot_nt(d_out_s, vals).astype(BF16).astype(F32)
            inner = jnp.sum(probs * d_probs, axis=-1, keepdims=True)
            d_scores = (probs * (d_probs - inner) * (HEAD_DIM ** -0.5)).astype(BF16)
            d_query = d_query + jnp.dot(d_scores, keys * mask, preferred_element_type=F32)
            d_keys = d_keys + dot_tn(d_scores, query_s)
            d_vals = d_vals + dot_tn(probs.astype(BF16), d_out_s)
        out_ref[:, 0, :, pl.ds(lo, PAIR)] = unrotate(d_query)
        out_ref[:, 0, :, pl.ds(lo_k, PAIR)] = unrotate(d_keys)
        out_ref[:, 0, :, pl.ds(lo_v, PAIR)] = d_vals.astype(BF16).reshape(SLOTS, ROWS, PAIR)
        return carry

    lax.fori_loop(0, HEADS // 2, body, 0)


def seq_block(width):
    return pl.BlockSpec((SLOTS, 1, ROWS, width), lambda s: (0, s, 0, 0))


def code_specs():
    return [pl.BlockSpec((1, SEQ, 1), lambda s: (s, 0, 0)), pl.BlockSpec((1, 1, SEQ), lambda s: (s, 0, 0))]


def attend(qkv, codes):
    seqs = qkv.shape[0] // SEQ
    return pl.pallas_call(
        attend_kernel,
        grid=(seqs,),
        in_specs=[seq_block(3 * D)] + code_specs(),
        out_specs=seq_block(D),
        out_shape=jax.ShapeDtypeStruct((SLOTS, seqs, ROWS, D), BF16),
        cost_estimate=pl.CostEstimate(flops=seqs * HEADS * 12 * SEQ * 65536 // 16, bytes_accessed=seqs * SEQ * D * 8, transcendentals=seqs * HEADS * SEQ * SEQ),
        name='attend',
    )(qkv.reshape(SLOTS, seqs, ROWS, 3 * D), codes[0], codes[1]).reshape(seqs * SEQ, D)


def attend_back(qkv, d_attn, codes, cosine, sine):
    seqs = qkv.shape[0] // SEQ
    return pl.pallas_call(
        attend_back_kernel,
        grid=(seqs,),
        in_specs=[seq_block(3 * D), seq_block(D)] + code_specs() + [seq_block(PAIR), seq_block(PAIR)],
        out_specs=seq_block(3 * D),
        out_shape=jax.ShapeDtypeStruct((SLOTS, seqs, ROWS, 3 * D), BF16),
        cost_estimate=pl.CostEstimate(flops=seqs * HEADS * 30 * SEQ * 65536 // 16, bytes_accessed=seqs * SEQ * D * 14, transcendentals=seqs * HEADS * SEQ * SEQ),
        name='attend_back',
    )(
        qkv.reshape(SLOTS, seqs, ROWS, 3 * D), d_attn.reshape(SLOTS, seqs, ROWS, D), codes[0], codes[1],
        cosine.reshape(SLOTS, seqs, ROWS, PAIR), sine.reshape(SLOTS, seqs, ROWS, PAIR),
    ).reshape(seqs * SEQ, 3 * D)


def rope_tables(positions):
    half = HEAD_DIM // 2
    inv_freq = ROPE_BASE ** (-jnp.arange(half, dtype=F32) / half)
    angles = positions.astype(F32)[:, None] * inv_freq
    cosine = jnp.cos(angles)
    sine = jnp.sin(angles)
    return jnp.concatenate([cosine] * 4, axis=1), jnp.concatenate([-sine, sine] * 2, axis=1)


def code_tables(code):
    seqs = code.shape[0] // SEQ
    ordered = code.reshape(SLOTS, seqs, ROWS).transpose(1, 0, 2)
    return ordered.reshape(seqs, SEQ, 1), ordered.reshape(seqs, 1, SEQ)


def block_forward(x, weights, tables, codes, block):
    gain_attn, qkv_w, out_w, gain_mlp, gate_w, up_w, down_w = weights
    normed, qkv = qkv_project(x, gain_attn, qkv_w, tables[0], tables[1], block)
    attn = attend(qkv, codes)
    mixed = jnp.dot(attn, out_w, preferred_element_type=F32)
    hidden = (x.astype(F32) + mixed).astype(BF16)
    normed_mlp, mlp_norm_pull = jax.vjp(rms_norm, hidden, gain_mlp)
    gate = jnp.dot(normed_mlp, gate_w, preferred_element_type=F32)
    upper = jnp.dot(normed_mlp, up_w, preferred_element_type=F32)
    activated, act_pull = jax.vjp(gated, gate, upper)
    mlp_out = jnp.dot(activated, down_w, preferred_element_type=F32)
    saved = dict(x=x, normed=normed, qkv=qkv, attn=attn, normed_mlp=normed_mlp, mlp_norm_pull=mlp_norm_pull, act_pull=act_pull, activated=activated)
    return mixed, hidden, mlp_out, saved


def halves(array, index):
    width = array.shape[1] // 2
    mine = lax.dynamic_slice_in_dim(array, index * width, width, axis=1)
    other = lax.dynamic_slice_in_dim(array, (1 - index) * width, width, axis=1)
    return mine, other


def swap(array):
    return lax.ppermute(array, 'cp', [(0, 1), (1, 0)])


def join_halves(mine, index):
    other = swap(mine)
    return jnp.where(index == 0, jnp.concatenate([mine, other], axis=1), jnp.concatenate([other, mine], axis=1))


def scatter(grad):
    return lax.psum_scatter(grad, 'fsdp', scatter_dimension=0, tiled=True)


def grad_plane_first(lhs, rhs, index):
    piece = scatter(dot_tn(lhs, rhs))
    mine, other = halves(piece, index)
    return join_halves((mine + swap(other)).astype(BF16), index)


def grad_pair_first(lhs, rhs, index):
    mine, other = halves(rhs, index)
    received = swap(dot_tn(lhs, other))
    return join_halves(scatter(dot_tn(lhs, mine) + received).astype(BF16), index)


def block_backward(saved, weights, tables, codes, d_mlp, d_hidden_extra, d_mixed_extra, index):
    gain_attn, qkv_w, out_w, gain_mlp, gate_w, up_w, down_w = weights
    d_act = dot_nt(d_mlp, down_w).astype(BF16)
    d_gate, d_upper = saved['act_pull'](d_act)
    d_gate = d_gate.astype(BF16)
    d_upper = d_upper.astype(BF16)
    g_down = grad_pair_first(saved['activated'], d_mlp, index)
    g_gate = grad_plane_first(saved['normed_mlp'], d_gate, index)
    g_up = grad_plane_first(saved['normed_mlp'], d_upper, index)
    d_normed_mlp = (dot_nt(d_gate, gate_w) + dot_nt(d_upper, up_w)).astype(BF16)
    d_hidden, g_gain_mlp = saved['mlp_norm_pull'](d_normed_mlp)
    if d_hidden_extra is not None:
        d_hidden = (d_hidden.astype(F32) + d_hidden_extra.astype(F32)).astype(BF16)
    d_mixed = d_hidden
    if d_mixed_extra is not None:
        d_mixed = (d_hidden.astype(F32) + d_mixed_extra.astype(F32)).astype(BF16)
    g_out = grad_pair_first(saved['attn'], d_mixed, index)
    d_attn = dot_nt(d_mixed, out_w).astype(BF16)
    d_qkv = attend_back(saved['qkv'], d_attn, codes, tables[0], tables[1])
    d_normed = dot_nt(d_qkv, qkv_w).astype(BF16)
    norm_pull = jax.vjp(rms_norm, saved['x'], gain_attn)[1]
    d_rows_norm, g_gain_attn = norm_pull(d_normed)
    d_rows = (d_hidden.astype(F32) + d_rows_norm.astype(F32)).astype(BF16)
    g_qkv = grad_plane_first(saved['normed'], d_qkv, index)
    return d_rows, (g_gain_attn, g_gain_mlp), (g_qkv, g_out, g_gate, g_up, g_down)


def solution(mesh):
    row_spec = P('fsdp', 'cp')
    weight_spec = P(None, 'fsdp')
    in_specs = (row_spec, P('fsdp'), P('fsdp'), weight_spec, weight_spec, weight_spec, weight_spec, weight_spec, weight_spec, weight_spec, row_spec)
    out_specs = (row_spec, row_spec, P('fsdp'), weight_spec, weight_spec, weight_spec, weight_spec, weight_spec, weight_spec, weight_spec)

    def local_step(hidden_in, select_pos, w_router, norm_attn, w_qkv, w_out, norm_mlp, w_gate, w_up, w_down, d_out):
        index = lax.axis_index('cp')
        fsdp_index = lax.axis_index('fsdp')
        batch = hidden_in.shape[0]
        seqs = batch // 2
        tokens = SLOTS * seqs * ROWS
        picks = select_pos.shape[1]

        def gather(shard):
            piece = lax.dynamic_slice_in_dim(shard, index * (shard.shape[0] // 2), shard.shape[0] // 2, axis=0)
            return lax.all_gather(piece, ('fsdp', 'cp'), axis=0, tiled=True)

        vectors = jnp.concatenate([norm_attn, norm_mlp, w_router[None]], axis=0)
        vectors = lax.all_gather(vectors, 'fsdp', axis=1, tiled=True)
        router_full = vectors[4].astype(F32)

        def gather_layer(layer):
            return (
                vectors[layer].astype(F32), gather(w_qkv[layer].reshape(-1, 3 * D)), gather(w_out[layer]), vectors[2 + layer].astype(F32),
                gather(w_gate[layer]), gather(w_up[layer]), gather(w_down[layer]),
            )

        def to_slots(array):
            keep = lax.dynamic_slice_in_dim(array, index * seqs, seqs, axis=0)
            send = lax.dynamic_slice_in_dim(array, (1 - index) * seqs, seqs, axis=0)
            return keep, swap(send)

        def from_slots(keep, send):
            received = swap(send)
            return jnp.where(index == 0, jnp.concatenate([keep, received], axis=0), jnp.concatenate([received, keep], axis=0))

        x_keep, x_recv = to_slots(hidden_in)
        x_rows = jnp.concatenate([x_keep, x_recv], axis=0).reshape(tokens, D)
        dy_slots = to_slots(d_out)
        chosen_pos = lax.dynamic_slice_in_dim(select_pos, index * seqs, seqs, axis=0)

        within = jnp.arange(ROWS, dtype=jnp.int32)
        slot_pos = (index * ROWS + within, (1 - index) * ROWS + within)
        row_pos = jnp.broadcast_to(jnp.stack(slot_pos)[:, None, :], (SLOTS, seqs, ROWS)).reshape(tokens)
        tables_one = rope_tables(row_pos)
        codes_one = code_tables(row_pos)
        pick_pos = chosen_pos.reshape(seqs * picks)
        tables_two = rope_tables(pick_pos)
        codes_two = code_tables((jnp.arange(seqs, dtype=jnp.int32)[:, None] * 256 + chosen_pos).reshape(seqs * picks))
        pick = [(chosen_pos[:, :, None] == pos[None, None, :]).astype(BF16) for pos in slot_pos]

        def choose(slots):
            parts = [jnp.einsum('bjt,btd->bjd', hot, rows, preferred_element_type=F32) for hot, rows in zip(pick, slots)]
            return (parts[0] + parts[1]).astype(BF16).reshape(seqs * picks, D)

        def place(rows, slot):
            return jnp.einsum('bjt,bjd->btd', pick[slot], rows.reshape(seqs, picks, D), preferred_element_type=F32)

        weights_one = gather_layer(0)
        weights_two = gather_layer(1)

        mixed, hidden, mlp_out, saved_one = block_forward(x_rows, weights_one, tables_one, codes_one, 768)
        first_out = (hidden.astype(F32) + mlp_out).astype(BF16)
        first_slots = first_out.reshape(SLOTS, seqs, ROWS, D)

        chosen = choose(first_slots)
        mixed_two, unused_hidden, mlp_two, saved_two = block_forward(chosen, weights_two, tables_two, codes_two, 192)
        delta = (mixed_two + mlp_two).astype(BF16)
        router = jnp.sum(chosen.astype(F32) * router_full, axis=-1, keepdims=True)
        updated = (chosen.astype(F32) + router * delta.astype(F32)).astype(BF16)
        out_slots = []
        for slot in range(SLOTS):
            selected = jnp.sum(pick[slot].astype(F32), axis=1) > 0
            out_slots.append(jnp.where(selected[:, :, None], place(updated, slot).astype(BF16), first_slots[slot]))
        hidden_out = from_slots(*out_slots)

        d_chosen = choose(dy_slots).astype(F32)
        d_delta = (router * d_chosen).astype(BF16)
        d_router = jnp.sum(d_chosen * delta.astype(F32), axis=-1, keepdims=True)
        d_rows_two, gains_two, grads_two = block_backward(saved_two, weights_two, tables_two, codes_two, d_delta, None, d_delta, index)
        g_router = jnp.sum(d_router * chosen.astype(F32), axis=0)
        d_total = (d_rows_two.astype(F32) + d_router * router_full).astype(BF16)
        d_first = jnp.concatenate([(dy_slots[slot].astype(F32) + place(d_total, slot)).astype(BF16) for slot in range(SLOTS)], axis=0).reshape(tokens, D)
        d_rows, gains_one, grads_one = block_backward(saved_one, weights_one, tables_one, codes_one, d_first, d_first, None, index)
        d_slots = d_rows.reshape(SLOTS, seqs, ROWS, D)
        d_hidden = from_slots(d_slots[0], d_slots[1])

        small = jnp.stack([gains_one[0], gains_two[0], gains_one[1], gains_two[1], g_router])
        small = lax.psum(small, ('cp', 'fsdp'))
        small = lax.dynamic_slice_in_dim(small, fsdp_index * (D // 8), D // 8, axis=1).astype(BF16)
        g_qkv, g_out, g_gate, g_up, g_down = [jnp.stack(pair) for pair in zip(grads_one, grads_two)]
        return (hidden_out, d_hidden, small[4], small[0:2], g_qkv.reshape(w_qkv.shape), g_out, small[2:4], g_gate, g_up, g_down)

    return jax.shard_map(local_step, mesh=mesh, in_specs=in_specs, out_specs=out_specs, check_vma=False)
```

```python
import functools

import jax
import jax.numpy as jnp
from jax import lax
from jax.experimental import pallas as pl
from jax.experimental.pallas import tpu as pltpu
from jax.sharding import Mesh, PartitionSpec as P


EPS = 1e-5
ROPE_BASE = 10000.0
F32 = jnp.float32
BF16 = jnp.bfloat16

D = 1024
FF = 4096
HEADS = 16
HEAD_DIM = 64
PAIR = 2 * HEAD_DIM
SLOTS = 2
ROWS = 96
SEQ = SLOTS * ROWS
BLOCKS = 8
NEAR = BLOCKS // 2
SCALE = HEAD_DIM ** -0.5
LOG2E = 1.4426950408889634
PARAMS = pltpu.CompilerParams(vmem_limit_bytes=60 * 1024 * 1024)


def cost(flops, traffic, transcendentals=0):
    return pl.CostEstimate(flops=int(flops), bytes_accessed=int(traffic), transcendentals=int(transcendentals))


def dot_nn(a, b):
    return lax.dot_general(a, b, (((1,), (0,)), ((), ())), preferred_element_type=F32)


def dot_nt(a, b):
    return lax.dot_general(a, b, (((1,), (1,)), ((), ())), preferred_element_type=F32)


def dot_tn(a, b):
    return lax.dot_general(a, b, (((0,), (0,)), ((), ())), preferred_element_type=F32)


def lane_block(k, parity, width=PAIR):
    return pl.ds(pl.multiple_of((2 * k + parity) * width, width), width)


def near_far(core):
    return (core, 1 - core)


def normed_parts(value_ref, gain_ref, inv_rms, core):
    parts = []
    for parity in near_far(core):
        pieces = []
        for k in range(NEAR):
            at = lane_block(k, parity)
            pieces.append((value_ref[:, at].astype(F32) * inv_rms * gain_ref[:, at]).astype(BF16))
        parts.append(jnp.concatenate(pieces, axis=1))
    return parts


def swap_halves(part):
    lane = lax.broadcasted_iota(jnp.int32, part.shape, part.ndim - 1)
    axis = part.ndim - 1
    return jnp.where(lane % HEAD_DIM < HEAD_DIM // 2, pltpu.roll(part, PAIR - HEAD_DIM // 2, axis), pltpu.roll(part, HEAD_DIM // 2, axis))


def qkv_kernel(core_ref, x_ref, gain_ref, wn_ref, wf_ref, cos_ref, sin_ref, *refs):
    near_ref, far_ref, out_ref = refs[-3:]
    core = core_ref[0]
    x_f = x_ref[...].astype(F32)
    inv_rms = lax.rsqrt(jnp.mean(x_f * x_f, axis=-1, keepdims=True) + EPS)
    near, far = normed_parts(x_ref, gain_ref, inv_rms, core)
    near_ref[...] = near
    far_ref[...] = far
    repeat = x_ref.shape[0] // cos_ref.shape[0]
    cosine = jnp.concatenate([cos_ref[...]] * repeat, axis=0)
    sine = jnp.concatenate([sin_ref[...]] * repeat, axis=0)
    width = 512
    for chunk in range(3 * D // width):
        cols = slice(chunk * width, (chunk + 1) * width)
        acc = dot_nn(near, wn_ref[:, cols]) + dot_nn(far, wf_ref[:, cols])
        if chunk * width < 2 * D:
            for j in range(width // PAIR):
                part = acc[:, j * PAIR:(j + 1) * PAIR]
                lo = chunk * width + j * PAIR
                out_ref[:, lo:lo + PAIR] = (part * cosine + swap_halves(part) * sine).astype(BF16)
        else:
            out_ref[:, cols] = acc.astype(BF16)


def resident(shape):
    return pl.BlockSpec(shape, lambda *_: (0,) * len(shape), pipeline_mode=pl.Buffered(1))


def rows_spec(block, width, first=0):
    return pl.BlockSpec((block, width), lambda i, core: (i + first, 0))


def in_place(carry, first_operand):
    specs = [pl.BlockSpec(memory_space=pl.ANY)] * len(carry)
    return specs, {first_operand + n: n for n in range(len(carry))}


def qkv_project(core, x, gain, w, tables, block, total, offset=0, slot=None, carry=()):
    rows = x.shape[0]
    first = offset // block
    table_spec = rows_spec(block, PAIR) if slot is None else pl.BlockSpec((ROWS, PAIR), lambda i, core: (slot, 0))
    carry_specs, aliases = in_place(carry, 7)
    return pl.pallas_call(
        qkv_kernel,
        grid_spec=pltpu.PrefetchScalarGridSpec(
            num_scalar_prefetch=1, grid=(rows // block,),
            in_specs=[rows_spec(block, D), resident((1, D)), resident((D // 2, 3 * D)), resident((D // 2, 3 * D)), table_spec, table_spec] + carry_specs,
            out_specs=[rows_spec(block, D // 2, first), rows_spec(block, D // 2, first), rows_spec(block, 3 * D, first)],
        ),
        out_shape=[jax.ShapeDtypeStruct((total, D // 2), BF16)] * 2 + [jax.ShapeDtypeStruct((total, 3 * D), BF16)],
        input_output_aliases=aliases,
        cost_estimate=cost(6 * rows * D * D, rows * D * 10 + 6 * D * D, rows),
        compiler_params=PARAMS,
        name='qkv_project',
    )(core, x, gain, w[0], w[1], *tables, *carry)


def attention_bias(col_ref, row_ref):
    code_k = col_ref[0]
    code_q = row_ref[0]
    allowed = (code_k <= code_q) & ((code_k >> 8) == (code_q >> 8))
    return jnp.where(allowed, 0.0, -1e30).astype(F32)


def load_pair(ref, lo):
    return ref[:, 0, :, pl.ds(lo, PAIR)].reshape(SEQ, PAIR)


def side_mask(side):
    lane = lax.broadcasted_iota(jnp.int32, (1, PAIR), 1)
    return (lane // HEAD_DIM == side).astype(F32).astype(BF16)


def probabilities(keys, query, bias):
    scores = dot_nt(keys, query) + bias
    top = jnp.max(scores, axis=0, keepdims=True)
    expo = jnp.exp2((scores - top) * (SCALE * LOG2E))
    return expo * (1.0 / jnp.sum(expo, axis=0, keepdims=True))


def attend_kernel(core_ref, qkv_ref, col_ref, row_ref, *refs):
    near_ref, far_ref = refs[-2:]
    bias = attention_bias(col_ref, row_ref)
    core = core_ref[0]
    masks = [side_mask(side) for side in range(2)]

    def body(k, carry):
        for parity, o_ref in zip(near_far(core), (near_ref, far_ref)):
            lo = (2 * k + parity) * PAIR
            query = load_pair(qkv_ref, pl.multiple_of(lo, PAIR))
            keys = load_pair(qkv_ref, pl.multiple_of(D + lo, PAIR))
            vals = load_pair(qkv_ref, pl.multiple_of(2 * D + lo, PAIR))
            out = None
            for mask in masks:
                probs = probabilities(keys * mask, query, bias).astype(BF16)
                term = dot_tn(probs, vals * mask)
                out = term if out is None else out + term
            o_ref[:, 0, :, pl.ds(pl.multiple_of(k * PAIR, PAIR), PAIR)] = out.astype(BF16).reshape(SLOTS, ROWS, PAIR)
        return carry

    lax.fori_loop(0, NEAR, body, 0)


def attend_back_kernel(core_ref, qkv_ref, near_ref, far_ref, col_ref, row_ref, cos_ref, sin_ref, out_ref):
    bias = attention_bias(col_ref, row_ref)
    core = core_ref[0]
    masks = [side_mask(side) for side in range(2)]
    cosine = cos_ref[:, 0].reshape(SEQ, PAIR)
    sine = sin_ref[:, 0].reshape(SEQ, PAIR)

    def unrotate(grad):
        part = grad.astype(BF16).astype(F32)
        return (part * cosine - swap_halves(part) * sine).astype(BF16).reshape(SLOTS, ROWS, PAIR)

    def body(k, carry):
        for parity, do_ref in zip(near_far(core), (near_ref, far_ref)):
            lo = (2 * k + parity) * PAIR
            lo_q = pl.multiple_of(lo, PAIR)
            lo_k = pl.multiple_of(D + lo, PAIR)
            lo_v = pl.multiple_of(2 * D + lo, PAIR)
            query = load_pair(qkv_ref, lo_q)
            keys = load_pair(qkv_ref, lo_k)
            vals = load_pair(qkv_ref, lo_v)
            d_out = load_pair(do_ref, pl.multiple_of(k * PAIR, PAIR))
            d_query = d_keys = d_vals = None
            for mask in masks:
                keys_s = keys * mask
                probs = probabilities(keys_s, query, bias)
                d_probs = dot_nt(vals * mask, d_out)
                inner = jnp.sum(probs * d_probs, axis=0, keepdims=True)
                d_scores = (probs * (d_probs - inner) * SCALE).astype(BF16)
                terms = (dot_tn(d_scores, keys_s), dot_nn(d_scores, query * mask), dot_nn(probs.astype(BF16), d_out * mask))
                if d_query is None:
                    d_query, d_keys, d_vals = terms
                else:
                    d_query, d_keys, d_vals = d_query + terms[0], d_keys + terms[1], d_vals + terms[2]
            out_ref[:, 0, :, pl.ds(lo_q, PAIR)] = unrotate(d_query)
            out_ref[:, 0, :, pl.ds(lo_k, PAIR)] = unrotate(d_keys)
            out_ref[:, 0, :, pl.ds(lo_v, PAIR)] = d_vals.astype(BF16).reshape(SLOTS, ROWS, PAIR)
        return carry

    lax.fori_loop(0, NEAR, body, 0)


def seq_block(width, shared=False, first=0):
    return pl.BlockSpec((SLOTS, 1, ROWS, width), lambda s, core: (0, 0 if shared else s + first, 0, 0))


def code_specs(codes):
    shared = codes[0].shape[0] == 1
    pick = lambda s, core: (0 if shared else s, 0, 0)
    return [pl.BlockSpec((1, SEQ, 1), pick), pl.BlockSpec((1, 1, SEQ), pick)]


def attend(core, qkv, codes, first=0, count=None, carry=()):
    seqs = qkv.shape[0] // SEQ
    count = count or seqs
    carry_specs, aliases = in_place(carry, 4)
    return pl.pallas_call(
        attend_kernel,
        grid_spec=pltpu.PrefetchScalarGridSpec(
            num_scalar_prefetch=1, grid=(count,), in_specs=[seq_block(3 * D, first=first)] + code_specs(codes) + carry_specs, out_specs=[seq_block(D // 2, first=first)] * 2,
        ),
        out_shape=[jax.ShapeDtypeStruct((SLOTS, seqs, ROWS, D // 2), BF16)] * 2,
        input_output_aliases=aliases,
        cost_estimate=cost(count * 2e9, count * SEQ * D * 8, count * HEADS * SEQ * SEQ),
        compiler_params=PARAMS,
        name='attend',
    )(core, qkv.reshape(SLOTS, seqs, ROWS, 3 * D), *codes, *carry)


def attend_back(core, qkv, d_attn, codes, tables):
    seqs = qkv.shape[0] // SEQ
    shared = tables[0].shape[0] == SEQ
    tables = [table.reshape(SLOTS, -1, ROWS, PAIR) for table in tables]
    return pl.pallas_call(
        attend_back_kernel,
        grid_spec=pltpu.PrefetchScalarGridSpec(
            num_scalar_prefetch=1, grid=(seqs,),
            in_specs=[seq_block(3 * D), seq_block(D // 2), seq_block(D // 2)] + code_specs(codes) + [seq_block(PAIR, shared)] * 2,
            out_specs=seq_block(3 * D),
        ),
        out_shape=jax.ShapeDtypeStruct((SLOTS, seqs, ROWS, 3 * D), BF16),
        cost_estimate=cost(seqs * 4.5e9, seqs * SEQ * D * 14, seqs * HEADS * SEQ * SEQ),
        compiler_params=PARAMS,
        name='attend_back',
    )(core, qkv.reshape(SLOTS, seqs, ROWS, 3 * D), *[part.reshape(SLOTS, seqs, ROWS, D // 2) for part in d_attn], *codes, *tables).reshape(seqs * SEQ, 3 * D)


def out_kernel(core_ref, on_ref, of_ref, wn_ref, wf_ref, x_ref, gain_ref, h_ref, near_ref, far_ref, *u_ref):
    mixed = dot_nn(on_ref[...], wn_ref[...]) + dot_nn(of_ref[...], wf_ref[...])
    if u_ref:
        u_ref[0][...] = mixed
    hidden = (x_ref[...].astype(F32) + mixed).astype(BF16)
    h_ref[...] = hidden
    h_f = hidden.astype(F32)
    inv_rms = lax.rsqrt(jnp.mean(h_f * h_f, axis=-1, keepdims=True) + EPS)
    near, far = normed_parts(h_ref, gain_ref, inv_rms, core_ref[0])
    near_ref[...] = near
    far_ref[...] = far


def out_project(core, attn, w, x, gain, block, keep_mixed):
    rows = x.shape[0]
    half = rows_spec(block, D // 2)
    full = rows_spec(block, D)
    extra = [full] if keep_mixed else []
    return pl.pallas_call(
        out_kernel,
        grid_spec=pltpu.PrefetchScalarGridSpec(
            num_scalar_prefetch=1, grid=(rows // block,),
            in_specs=[half, half, resident((D // 2, D)), resident((D // 2, D)), full, resident((1, D))],
            out_specs=[full, half, half] + extra,
        ),
        out_shape=[jax.ShapeDtypeStruct((rows, D), BF16)] + [jax.ShapeDtypeStruct((rows, D // 2), BF16)] * 2 + [jax.ShapeDtypeStruct((rows, D), F32)] * len(extra),
        cost_estimate=cost(2 * rows * D * D, rows * D * 8 + 2 * D * D, rows),
        compiler_params=PARAMS,
        name='out_project',
    )(core, *attn, *w, x, gain)


def real_block(j, core):
    return 2 * lax.rem(j, NEAR) + jnp.where(j < NEAR, core, 1 - core)


def gate_up_kernel(core_ref, near_ref, far_ref, gn_ref, gf_ref, un_ref, uf_ref, gate_ref, up_ref, an_ref, af_ref):
    near = near_ref[...]
    far = far_ref[...]
    gate = dot_nn(near, gn_ref[...]) + dot_nn(far, gf_ref[...])
    upper = dot_nn(near, un_ref[...]) + dot_nn(far, uf_ref[...])
    gate_ref[...] = gate
    up_ref[...] = upper
    act = (gate * lax.logistic(gate) * upper).astype(BF16)
    j = pl.program_id(1)

    @pl.when(j < NEAR)
    def _():
        an_ref[...] = act

    @pl.when(j >= NEAR)
    def _():
        af_ref[...] = act


def gate_up(core, normed, gate_w, up_w, block):
    rows = normed[0].shape[0]
    tile = FF // BLOCKS
    half = pl.BlockSpec((block, D // 2), lambda i, j, core: (i, 0))
    weight = pl.BlockSpec((D // 2, tile), lambda i, j, core: (0, real_block(j, core[0])))
    value = pl.BlockSpec((block, tile), lambda i, j, core: (i, real_block(j, core[0])))
    near = pl.BlockSpec((block, tile), lambda i, j, core: (i, jnp.minimum(j, NEAR - 1)))
    far = pl.BlockSpec((block, tile), lambda i, j, core: (i, jnp.maximum(j - NEAR, 0)))
    return pl.pallas_call(
        gate_up_kernel,
        grid_spec=pltpu.PrefetchScalarGridSpec(
            num_scalar_prefetch=1, grid=(rows // block, BLOCKS), in_specs=[half, half] + [weight] * 4, out_specs=[value, value, near, far],
        ),
        out_shape=[jax.ShapeDtypeStruct((rows, FF), F32)] * 2 + [jax.ShapeDtypeStruct((rows, FF // 2), BF16)] * 2,
        cost_estimate=cost(4 * rows * D * FF, rows * (FF * 10 + D * 2) + 4 * D * FF, rows * FF),
        compiler_params=PARAMS,
        name='gate_up',
    )(core, *normed, *gate_w, *up_w)


def down_kernel(an_ref, af_ref, wn_ref, wf_ref, res_ref, out_ref):
    out = dot_nn(an_ref[...], wn_ref[...]) + dot_nn(af_ref[...], wf_ref[...])
    out_ref[...] = (res_ref[...].astype(F32) + out).astype(BF16)


def down_project(act, w, residual, block):
    rows = residual.shape[0]
    half = pl.BlockSpec((block, FF // 2), lambda i: (i, 0))
    full = pl.BlockSpec((block, D), lambda i: (i, 0))
    return pl.pallas_call(
        down_kernel,
        grid=(rows // block,),
        in_specs=[half, half, resident((FF // 2, D)), resident((FF // 2, D)), full],
        out_specs=full,
        out_shape=jax.ShapeDtypeStruct((rows, D), BF16),
        cost_estimate=cost(2 * rows * D * FF, rows * (FF * 2 + D * 4) + 2 * D * FF),
        compiler_params=PARAMS,
        name='down_project',
    )(*act, *w, residual)


def act_back_kernel(core_ref, dm_ref, wn_ref, wf_ref, gate_ref, up_ref, dg_ref, du_ref):
    def finish(w_ref):
        d_act = dot_nt(dm_ref[...], w_ref[...]).astype(BF16).astype(F32)
        gate = gate_ref[...]
        sig = lax.logistic(gate)
        dg_ref[...] = (d_act * up_ref[...] * (sig * (1.0 + gate * (1.0 - sig)))).astype(BF16)
        du_ref[...] = (d_act * (gate * sig)).astype(BF16)

    j = pl.program_id(1)

    @pl.when(j < NEAR)
    def _():
        finish(wn_ref)

    @pl.when(j >= NEAR)
    def _():
        finish(wf_ref)


def act_back(core, d_mlp, w, gate, upper, block):
    rows = d_mlp.shape[0]
    tile = FF // BLOCKS
    value = pl.BlockSpec((block, tile), lambda i, j, core: (i, real_block(j, core[0])))
    return pl.pallas_call(
        act_back_kernel,
        grid_spec=pltpu.PrefetchScalarGridSpec(
            num_scalar_prefetch=1, grid=(rows // block, BLOCKS),
            in_specs=[
                pl.BlockSpec((block, D), lambda i, j, core: (i, 0)),
                pl.BlockSpec((tile, D), lambda i, j, core: (jnp.minimum(j, NEAR - 1), 0)),
                pl.BlockSpec((tile, D), lambda i, j, core: (jnp.maximum(j - NEAR, 0), 0)),
                value, value,
            ],
            out_specs=[value, value],
        ),
        out_shape=[jax.ShapeDtypeStruct((rows, FF), BF16)] * 2,
        cost_estimate=cost(3 * rows * D * FF, rows * (FF * 12 + D * 2) + 2 * D * FF, rows * FF),
        compiler_params=PARAMS,
        name='act_back',
    )(core, d_mlp, *w, gate, upper)


def norm_back_kernel(pairs, plain, core_ref, *refs):
    grads = [refs[3 * p:3 * p + 3] for p in range(pairs)]
    value_ref, extra_ref, gain_ref, out_ref = refs[3 * pairs:3 * pairs + 4]
    rest = refs[3 * pairs + 4:]
    plain_ref = rest[0] if plain else None
    gain_out_ref, acc_ref = rest[-2:]
    core = core_ref[0]
    i = pl.program_id(0)
    k = pl.program_id(1)
    for index, parity in enumerate(near_far(core)):
        total = None
        for group in grads:
            term = dot_nt(group[0][...], group[1 + index][...])
            total = term if total is None else total + term

        @pl.when(k == 0)
        def _():
            for b in range(NEAR):
                acc_ref[:, lane_block(b, parity)] = total[:, b * PAIR:(b + 1) * PAIR]

        @pl.when(k > 0)
        def _():
            for b in range(NEAR):
                acc_ref[:, lane_block(b, parity)] += total[:, b * PAIR:(b + 1) * PAIR]

    @pl.when(k == pl.num_programs(1) - 1)
    def _():
        chunk = 64
        gain = gain_ref[...]

        def step(s, sums):
            at = pl.ds(pl.multiple_of(s * chunk, chunk), chunk)
            d_normed = acc_ref[at, :].astype(BF16).astype(F32)
            value = value_ref[at, :].astype(F32)
            inv_rms = lax.rsqrt(jnp.mean(value * value, axis=-1, keepdims=True) + EPS)
            scaled = d_normed * gain
            inner = jnp.sum(scaled * value, axis=-1, keepdims=True) * (inv_rms * inv_rms * inv_rms * (1.0 / D))
            d_value = (scaled * inv_rms - value * inner).astype(BF16)
            if plain:
                plain_ref[at, :] = d_value
            out_ref[at, :] = (d_value.astype(F32) + extra_ref[at, :].astype(F32)).astype(BF16)
            unit = d_normed * (value * inv_rms)
            return sums + jnp.sum(unit.reshape(chunk // 8, 8, D), axis=0)

        sums = lax.fori_loop(0, out_ref.shape[0] // chunk, step, jnp.zeros((8, D), F32))

        @pl.when(i == 0)
        def _():
            gain_out_ref[...] = sums

        @pl.when(i > 0)
        def _():
            gain_out_ref[...] += sums


def norm_back(core, grads, weights, value, extra, gain, block, tile, plain, offset=0, rows=None):
    rows = rows or value.shape[0]
    first = offset // block
    steps = grads[0].shape[1] // tile
    full = pl.BlockSpec((block, D), lambda i, k, core: (i, 0))
    source = pl.BlockSpec((block, D), lambda i, k, core: (i + first, 0))
    in_specs, operands = [], []
    for grad, weight in zip(grads, weights):
        in_specs += [pl.BlockSpec((block, tile), lambda i, k, core: (i + first, k))] + [pl.BlockSpec((D // 2, tile), lambda i, k, core: (0, k))] * 2
        operands += [grad, *weight]
    outs = 2 if plain else 1
    result = pl.pallas_call(
        functools.partial(norm_back_kernel, len(grads), plain),
        grid_spec=pltpu.PrefetchScalarGridSpec(
            num_scalar_prefetch=1, grid=(rows // block, steps),
            in_specs=in_specs + [source, source, resident((1, D))],
            out_specs=[full] * outs + [pl.BlockSpec((8, D), lambda i, k, core: (0, 0))],
            scratch_shapes=[pltpu.VMEM((block, D), F32)],
        ),
        out_shape=[jax.ShapeDtypeStruct((rows, D), BF16)] * outs + [jax.ShapeDtypeStruct((8, D), F32)],
        cost_estimate=cost(2 * rows * D * steps * tile * len(grads), rows * steps * tile * 2 * len(grads) + rows * D * 6, rows),
        compiler_params=PARAMS,
    )(core, *operands, value, extra, gain)
    return result[:-1], jnp.sum(result[-1], axis=0)


def rope_tables(positions):
    half = HEAD_DIM // 2
    inv_freq = ROPE_BASE ** (-jnp.arange(half, dtype=F32) / half)
    angles = positions.astype(F32)[:, None] * inv_freq
    cosine = jnp.cos(angles)
    sine = jnp.sin(angles)
    return jnp.concatenate([cosine] * 4, axis=1), jnp.concatenate([-sine, sine] * 2, axis=1)


def code_tables(code):
    seqs = code.shape[0] // SEQ
    ordered = code.reshape(SLOTS, seqs, ROWS).transpose(1, 0, 2)
    return ordered.reshape(seqs, SEQ, 1), ordered.reshape(seqs, 1, SEQ)


def after(value, *earlier):
    return lax.optimization_barrier((value,) + tuple(earlier))[0]


def swap(array, axis):
    return lax.ppermute(array, axis, [(0, 1), (1, 0)])


def halves(array, index):
    width = array.shape[1] // 2
    mine = lax.dynamic_slice_in_dim(array, index * width, width, axis=1)
    other = lax.dynamic_slice_in_dim(array, (1 - index) * width, width, axis=1)
    return mine, other


def join_halves(mine, index):
    other = swap(mine, 'z')
    return jnp.where(index == 0, jnp.concatenate([mine, other], axis=1), jnp.concatenate([other, mine], axis=1))


def scatter(grad):
    return lax.psum_scatter(grad, ('y', 'x'), scatter_dimension=0, tiled=True)


def plane_grad(lhs, rhs, *earlier):
    far = dot_tn(lhs[1], after(rhs, *earlier))
    received = swap(far, 'c')

    def near(*earlier):
        return dot_tn(lhs[0], after(rhs, *earlier)) + received

    return far, near


def plane_finish(total, index):
    mine, other = halves(scatter(total), index)
    return join_halves((mine + swap(other, 'z')).astype(BF16), index)


def stack_grad(lhs, rhs, index, *earlier):
    mine, other = halves(after(rhs, *earlier), index)
    far_other = dot_tn(lhs[1], other)
    far_mine = dot_tn(lhs[1], after(mine, far_other))
    got_other = swap(far_other, 'c')
    got_mine = swap(far_mine, 'c')

    def near_other(*earlier):
        sent = dot_tn(lhs[0], after(other, *earlier)) + got_other
        return sent, swap(sent, 'z')

    def near_mine(received, *earlier):
        return dot_tn(lhs[0], after(mine, *earlier)) + got_mine + received

    return (far_other, far_mine), near_other, near_mine


def stack_finish(total, index):
    return join_halves(scatter(total).astype(BF16), index)


def paired(near, *earlier):
    return near, swap(after(near, *earlier), 'c')


def block_forward(core, x, weights, tables, codes, routed, early):
    gain_attn, qkv_w, out_w, gain_mlp, gate_w, up_w, down_w = weights
    small = x.shape[0] < 1024
    qkv_w = paired(qkv_w, *early['qkv'])
    if routed:
        near, far, qkv = qkv_project(core, x, gain_attn, qkv_w, tables, 192, x.shape[0])
        out_w = paired(out_w, *early['out'])
        attn = attend(core, qkv, codes)
    else:
        keep, first, second = early['parts']
        total = x.shape[0]
        count = total // SEQ // 2
        carry = qkv_project(core, keep, gain_attn, qkv_w, tables, 384, total, 0, 0)
        near, far, qkv = qkv_project(core, first, gain_attn, qkv_w, tables, 384, total, total // 2, 1, carry)
        attn = attend(core, qkv, codes, 0, count)
        out_w = paired(out_w, near)
        near, far, qkv = qkv_project(core, after(second, *attn), gain_attn, qkv_w, tables, 384, total, total // 2 + count * ROWS, 1, (near, far, qkv))
        attn = attend(core, qkv, codes, count, count, attn)
    attn = [part.reshape(x.shape[0], D // 2) for part in attn]
    gate_w = paired(gate_w, *early.get('mlp', (attn[0],)))
    up_w = paired(up_w, *early.get('mlp', (attn[0],)))
    hidden, m_near, m_far, *mixed = out_project(core, attn, out_w, x, gain_mlp, 192 if small else 768, routed)
    down_w = paired(down_w, hidden)
    gate, upper, a_near, a_far = gate_up(core, (m_near, m_far), gate_w, up_w, 384 if small else 1536)
    result = down_project((a_near, a_far), down_w, mixed[0] if routed else hidden, 192 if small else 384)
    saved = dict(x=x, normed=(near, far), qkv=qkv, attn=attn, hidden=hidden, normed_mlp=(m_near, m_far), gate=gate, upper=upper, act=(a_near, a_far))
    saved['weights'] = (gain_attn, qkv_w, out_w, gain_mlp, gate_w, up_w, down_w)
    return result, saved


def solution(mesh):
    mesh = Mesh(mesh.devices.reshape(2, 2, 2, 2), ('z', 'y', 'x', 'c'))
    fsdp = ('y', 'x', 'c')
    row_spec = P(fsdp, 'z')
    weight_spec = P(None, fsdp)
    in_specs = (row_spec, P(fsdp), P(fsdp), weight_spec, weight_spec, weight_spec, weight_spec, weight_spec, weight_spec, weight_spec, row_spec)
    out_specs = (row_spec, row_spec, P(fsdp), weight_spec, weight_spec, weight_spec, weight_spec, weight_spec, weight_spec, weight_spec)

    def local_step(hidden_in, select_pos, w_router, norm_attn, w_qkv, w_out, norm_mlp, w_gate, w_up, w_down, d_out):
        index = lax.axis_index('z')
        core_index = lax.axis_index('c')
        core = core_index.reshape(1).astype(jnp.int32)
        fsdp_index = lax.axis_index(fsdp)
        seqs = hidden_in.shape[0] // 2
        tokens = SLOTS * seqs * ROWS
        picks = select_pos.shape[1]

        def gather(shard, name):
            if name in ('qkv0', 'out0'):
                return lax.all_gather(shard, ('y', 'x'), axis=0, tiled=True)
            rows = shard.shape[0] // 2
            piece = lax.dynamic_slice_in_dim(shard, index * rows, rows, axis=0)
            return lax.all_gather(piece, ('y', 'x', 'z'), axis=0, tiled=True)

        vectors = jnp.concatenate([norm_attn, norm_mlp, w_router[None]], axis=0)
        vectors = lax.all_gather(vectors, fsdp, axis=1, tiled=True).astype(F32)
        router_full = vectors[4]

        def gather_layer(layer):
            return (
                vectors[layer][None], gather(w_qkv[layer].reshape(-1, 3 * D), f'qkv{layer}'), gather(w_out[layer], f'out{layer}'), vectors[2 + layer][None],
                gather(w_gate[layer], f'gate{layer}'), gather(w_up[layer], f'up{layer}'), gather(w_down[layer], f'down{layer}'),
            )

        def keep_send(array):
            return (lax.dynamic_slice_in_dim(array, index * seqs, seqs, axis=0), lax.dynamic_slice_in_dim(array, (1 - index) * seqs, seqs, axis=0))

        def from_slots(keep, received):
            return jnp.where(index == 0, jnp.concatenate([keep, received], axis=0), jnp.concatenate([received, keep], axis=0))

        within = jnp.arange(ROWS, dtype=jnp.int32)
        slot_pos = (index * ROWS + within, (1 - index) * ROWS + within)
        row_pos = jnp.concatenate(slot_pos)
        tables_one = rope_tables(row_pos)
        codes_one = code_tables(row_pos)
        chosen_pos = lax.dynamic_slice_in_dim(select_pos, index * seqs, seqs, axis=0)
        tables_two = rope_tables(chosen_pos.reshape(seqs * picks))
        codes_two = code_tables((jnp.arange(seqs, dtype=jnp.int32)[:, None] * 256 + chosen_pos).reshape(seqs * picks))
        pick = [(chosen_pos[:, :, None] == pos[None, None, :]).astype(BF16) for pos in slot_pos]

        def choose(slots):
            parts = [jnp.einsum('bjt,btd->bjd', hot, rows, preferred_element_type=F32) for hot, rows in zip(pick, slots)]
            return (parts[0] + parts[1]).astype(BF16).reshape(seqs * picks, D)

        def place(rows, slot):
            return jnp.einsum('bjt,bjd->btd', pick[slot], rows.reshape(seqs, picks, D), preferred_element_type=F32)

        x_keep, x_send = keep_send(hidden_in)
        x_parts = [x_keep] + [swap(x_send[n * (seqs // 2):(n + 1) * (seqs // 2)], 'z') for n in range(2)]
        x_rows = jnp.concatenate(x_parts, axis=0).reshape(tokens, D)
        x_parts = [part.reshape(-1, D) for part in x_parts]
        weights_one = gather_layer(0)
        weights_two = gather_layer(1)

        first_out, one = block_forward(core, x_rows, weights_one, tables_one, codes_one, False, dict(qkv=(), parts=x_parts))
        weights_one = one['weights']
        dy_keep, dy_send = keep_send(after(d_out, one['qkv']))
        dy_slots = (dy_keep, swap(dy_send, 'z'))
        first_slots = first_out.reshape(SLOTS, seqs, ROWS, D)
        chosen = choose(first_slots)
        delta, two = block_forward(core, chosen, weights_two, tables_two, codes_two, True, dict(qkv=(one['act'][0],), out=(one['act'][0],), mlp=(first_out,)))
        weights_two = two['weights']
        router = jnp.sum(chosen.astype(F32) * router_full, axis=-1, keepdims=True)
        updated = (chosen.astype(F32) + router * delta.astype(F32)).astype(BF16)
        out_slots = []
        for slot in range(SLOTS):
            selected = jnp.sum(pick[slot].astype(F32), axis=1) > 0
            out_slots.append(jnp.where(selected[:, :, None], place(updated, slot).astype(BF16), first_slots[slot]))
        out_received = swap(out_slots[1], 'z')

        d_chosen = choose(dy_slots).astype(F32)
        d_delta = (router * d_chosen).astype(BF16)
        d_router = jnp.sum(d_chosen * delta.astype(F32), axis=-1, keepdims=True)
        g_router = jnp.sum(d_router * chosen.astype(F32), axis=0)

        def mlp_grads(saved, weights, d_mlp, block):
            d_gate, d_upper = act_back(core, d_mlp, weights[6], saved['gate'], saved['upper'], block)
            down_far, down_other, down_mine = stack_grad(saved['act'], d_mlp, index, d_gate)
            gate_far, gate_near = plane_grad(saved['normed_mlp'], d_gate, *down_far)
            up_far, up_near = plane_grad(saved['normed_mlp'], d_upper, gate_far)
            down_sent, down_received = down_other(up_far)
            gate_total = gate_near(down_sent)
            up_total = up_near(gate_total)
            return (d_gate, d_upper), (down_received, down_mine), gate_total, up_total

        gains2 = (weights_two[0], weights_two[3])
        d_mid2, down2, gate2_total, up2_total = mlp_grads(two, weights_two, d_delta, 384)
        g_gate2 = plane_finish(gate2_total, index)
        g_up2 = plane_finish(up2_total, index)
        (d_mixed2, d_hidden2), gain_mlp2 = norm_back(core, (after(d_mid2[0], up2_total), d_mid2[1]), (weights_two[4], weights_two[5]), two['hidden'], d_delta, gains2[1], 384, 512, True)
        out2_far, out2_other, out2_mine = stack_grad(two['attn'], d_mixed2, index)
        d_attn2 = [dot_nt(after(d_mixed2, *out2_far), w).astype(BF16) for w in weights_two[2]]
        d_qkv2 = attend_back(core, two['qkv'], d_attn2, codes_two, tables_two)
        qkv2_far, qkv2_near = plane_grad(two['normed'], d_qkv2)
        out2_sent, out2_received = out2_other(qkv2_far)
        (d_rows2,), gain_attn2 = norm_back(core, (after(d_qkv2, out2_sent),), (weights_two[1],), two['x'], d_hidden2, gains2[0], 384, 1024, False)
        qkv2_total = qkv2_near(d_rows2)
        g_qkv2 = plane_finish(qkv2_total, index)

        d_total = (d_rows2.astype(F32) + d_router * router_full).astype(BF16)
        d_total = after(d_total, qkv2_total, out_slots[1])
        d_first = jnp.concatenate([(dy_slots[slot].astype(F32) + place(d_total, slot)).astype(BF16) for slot in range(SLOTS)], axis=0).reshape(tokens, D)

        gains1 = (weights_one[0], weights_one[3])
        d_mid1, down1, gate1_total, up1_total = mlp_grads(one, weights_one, d_first, 1536)
        g_gate1 = plane_finish(gate1_total, index)
        g_up1 = plane_finish(up1_total, index)
        down2_total = down2[1](down2[0], up1_total)
        g_down2 = stack_finish(down2_total, index)
        out2_total = out2_mine(out2_received, down2_total)
        g_out2 = stack_finish(out2_total, index)
        (d_hidden1,), gain_mlp1 = norm_back(core, (after(d_mid1[0], out2_total), d_mid1[1]), (weights_one[4], weights_one[5]), one['hidden'], d_first, gains1[1], 768, 1024, False)
        out1_far, out1_other, out1_mine = stack_grad(one['attn'], d_hidden1, index)
        d_attn1 = [dot_nt(after(d_hidden1, *out1_far), w).astype(BF16) for w in weights_one[2]]
        out1_sent, out1_received = out1_other(*d_attn1)
        down1_total = down1[1](down1[0], out1_sent)
        g_down1 = stack_finish(down1_total, index)
        d_qkv1 = attend_back(core, one['qkv'], [after(d_attn1[0], down1_total), d_attn1[1]], codes_one, tables_one)
        qkv1_far, qkv1_near = plane_grad(one['normed'], d_qkv1)

        def last_back(d_qkv, slot):
            rows = tokens // SLOTS
            return norm_back(core, (d_qkv,), (weights_one[1],), one['x'], d_hidden1, gains1[0], 768, 1024, False, slot * rows, rows)

        (d_send,), gain_attn1 = last_back(after(d_qkv1, qkv1_far), 1)
        d_received = swap(d_send.reshape(seqs, ROWS, D), 'z')
        qkv1_total = qkv1_near(d_send)
        g_qkv1 = plane_finish(qkv1_total, index)
        (d_keep,), gain_more = last_back(after(d_qkv1, qkv1_total), 0)
        gain_attn1 = gain_attn1 + gain_more
        out1_total = out1_mine(out1_received, d_keep)
        g_out1 = stack_finish(out1_total, index)
        d_hidden = from_slots(d_keep.reshape(seqs, ROWS, D), d_received)
        hidden_out = from_slots(out_slots[0], out_received)

        small = jnp.stack([gain_attn1, gain_attn2, gain_mlp1, gain_mlp2, g_router])
        for axis in ('c', 'x', 'y', 'z'):
            small = small + swap(small, axis)
        small = lax.dynamic_slice_in_dim(small, fsdp_index * (D // 8), D // 8, axis=1).astype(BF16)
        stack = lambda one_part, two_part: jnp.stack([one_part, two_part])
        return (
            hidden_out, d_hidden, small[4], small[0:2], stack(g_qkv1, g_qkv2).reshape(w_qkv.shape), stack(g_out1, g_out2), small[2:4],
            stack(g_gate1, g_gate2), stack(g_up1, g_up2), stack(g_down1, g_down2),
        )

    return jax.shard_map(local_step, mesh=mesh, in_specs=in_specs, out_specs=out_specs, check_vma=False)
```
